8 devices in a mesh: sp: 8 (over z, y, x, core).
Axes of the slice: x: 2, y: 2, z: 1, core: 2. Of those that a mesh axis runs over, the one named last changes fastest.
Arguments:
- x: bfloat16 [32, 1024, 2048], P(None, 'sp')
- dy: bfloat16 [32, 1024, 2048], P(None, 'sp')
- prefix_len: int32 [32], replicated
- w_norm: bfloat16 [2048], replicated
- w_q: bfloat16 [2048, 2048], replicated
- w_k: bfloat16 [2048, 128], replicated
- w_v: bfloat16 [2048, 128], replicated
- w_o: bfloat16 [2048, 2048], replicated
Outputs:
- output 1: bfloat16 [32, 1024, 2048], P(None, 'sp')
- output 2: bfloat16 [32, 1024, 2048], P(None, 'sp')
- output 3: float32 [2048, 2048], replicated
- output 4: float32 [2048, 128], replicated
- output 5: float32 [2048, 128], replicated
- output 6: float32 [2048, 2048], replicated
- output 7: float32 [2048], replicated
All inputs are finite; a program needn't handle non-finite values.
Results may differ from the reference program's by a relative error of at most 0.0115518.
Values are sent between devices in bfloat16 or wider.
A program may use at most 1 GiB of HBM per device.

```python
import math
import functools
import jax
import jax.numpy as jnp
from jax import lax

BATCH = 32
SEQ_LEN = 1024
D_MODEL = 2048
HEADS = 16
HEAD_DIM = 128

ROPE_THETA = 10000.0
NORM_EPS = 1e-6
MASK_FILL = -1e30
ROW_BLOCK = math.gcd(SEQ_LEN, 256)


def setup_inputs(seed: int = 0) -> dict:
    keys = jax.random.split(jax.random.key(seed), 9)
    q_width = HEADS * HEAD_DIM
    x = jax.random.normal(keys[0], (BATCH, SEQ_LEN, D_MODEL), jnp.float32)
    dy = jax.random.normal(keys[1], (BATCH, SEQ_LEN, D_MODEL), jnp.float32)
    prefix_low = SEQ_LEN // 8
    prefix_high = 7 * SEQ_LEN // 8
    drawn_lens = jax.random.randint(keys[2], (BATCH,), prefix_low, prefix_high + 1, dtype=jnp.int32)
    drawn_lens = drawn_lens.at[0].set(prefix_low).at[1].set(prefix_high)
    prefix_len = jax.random.permutation(keys[3], drawn_lens)
    w_norm = 0.5 * jax.random.normal(keys[4], (D_MODEL,), jnp.float32)
    w_q = 1.2 * D_MODEL ** -0.5 * jax.random.normal(keys[5], (D_MODEL, q_width), jnp.float32)
    w_k = 1.2 * D_MODEL ** -0.5 * jax.random.normal(keys[6], (D_MODEL, HEAD_DIM), jnp.float32)
    w_v = D_MODEL ** -0.5 * jax.random.normal(keys[7], (D_MODEL, HEAD_DIM), jnp.float32)
    w_o = 2.0 * q_width ** -0.5 * jax.random.normal(keys[8], (q_width, D_MODEL), jnp.float32)
    return {'x': x.astype(jnp.bfloat16), 'dy': dy.astype(jnp.bfloat16), 'prefix_len': prefix_len, 'w_norm': w_norm.astype(jnp.bfloat16), 'w_q': w_q.astype(jnp.bfloat16), 'w_k': w_k.astype(jnp.bfloat16), 'w_v': w_v.astype(jnp.bfloat16), 'w_o': w_o.astype(jnp.bfloat16)}


def to_bf16_grid(values):
    return values.astype(jnp.bfloat16).astype(jnp.float32)


def rope_tables(positions):
    half = HEAD_DIM // 2
    frequencies = ROPE_THETA ** (-2.0 * jnp.arange(half, dtype=jnp.float32) / HEAD_DIM)
    angles = positions.astype(jnp.float32)[:, None] * frequencies[None, :]
    return jnp.cos(angles), jnp.sin(angles)


def apply_rope(vectors, cos_tab, sin_tab):
    half = vectors.shape[-1] // 2
    first = vectors[..., :half]
    second = vectors[..., half:]
    return jnp.concatenate([first * cos_tab - second * sin_tab, second * cos_tab + first * sin_tab], axis=-1)


def attend_sequence(item):
    q_seq, k_seq, v_seq, prefix = item
    key_pos = jnp.arange(SEQ_LEN)

    def one_block(block_item):
        q_rows, start = block_item
        row_pos = start + jnp.arange(ROW_BLOCK)
        visible = (key_pos[None, :] < prefix) | (key_pos[None, :] <= row_pos[:, None])
        scores = jnp.einsum('qhe,ke->hqk', q_rows, k_seq)
        scores = jnp.where(visible[None], scores, MASK_FILL)
        attn_probs = to_bf16_grid(jax.nn.softmax(scores, axis=-1))
        return to_bf16_grid(jnp.einsum('hqk,ke->qhe', attn_probs, v_seq))

    blocks = q_seq.reshape(SEQ_LEN // ROW_BLOCK, ROW_BLOCK, HEADS, HEAD_DIM)
    starts = jnp.arange(SEQ_LEN // ROW_BLOCK) * ROW_BLOCK
    attn_out = lax.map(jax.checkpoint(one_block), (blocks, starts))
    return attn_out.reshape(SEQ_LEN, HEADS, HEAD_DIM)


def block_forward(x, gain, w_q, w_k, w_v, w_o, prefix_len):
    x_f32 = x.astype(jnp.float32)
    inv_rms = lax.rsqrt(jnp.mean(x_f32 * x_f32, axis=-1, keepdims=True) + NORM_EPS)
    normed = to_bf16_grid(x_f32 * inv_rms * (1.0 + gain))
    cos_tab, sin_tab = rope_tables(jnp.arange(SEQ_LEN))
    q_proj = jnp.einsum('bsd,de->bse', normed, w_q).reshape(BATCH, SEQ_LEN, HEADS, HEAD_DIM)
    queries = to_bf16_grid(apply_rope(q_proj, cos_tab[:, None, :], sin_tab[:, None, :]) * HEAD_DIM ** -0.5)
    keys = to_bf16_grid(apply_rope(jnp.einsum('bsd,de->bse', normed, w_k), cos_tab, sin_tab))
    values = to_bf16_grid(jnp.einsum('bsd,de->bse', normed, w_v))
    attn_out = lax.map(attend_sequence, (queries, keys, values, prefix_len))
    mixed = jnp.einsum('bse,ed->bsd', attn_out.reshape(BATCH, SEQ_LEN, HEADS * HEAD_DIM), w_o)
    return (x_f32 + mixed).astype(jnp.bfloat16)


def reference(x, dy, prefix_len, w_norm, w_q, w_k, w_v, w_o):
    forward = functools.partial(block_forward, prefix_len=prefix_len)
    y_out, pull_back = jax.vjp(forward, x, w_norm.astype(jnp.float32), w_q.astype(jnp.float32), w_k.astype(jnp.float32), w_v.astype(jnp.float32), w_o.astype(jnp.float32))
    dx_out, d_gain, d_wq, d_wk, d_wv, d_wo = pull_back(dy)
    return y_out, dx_out, d_wq, d_wk, d_wv, d_wo, d_gain
```

```python
import functools

import jax
import jax.numpy as jnp
from jax import lax
from jax.experimental import pallas as pl
from jax.experimental.pallas import tpu as pltpu
from jax.sharding import PartitionSpec as P


ROPE_THETA = 10000.0
NORM_EPS = 1e-6
MASK_FILL = -1e30
F32 = jnp.float32
BF16 = jnp.bfloat16
MESH = pl.DeviceIdType.MESH
VMEM_LIMIT = 60 * 1024 * 1024
NT = (((1,), (1,)), ((), ()))


def mm(a, b):
    return jnp.dot(a, b, preferred_element_type=F32)


def mm_nt(a, b):
    return lax.dot_general(a, b, NT, preferred_element_type=F32)


def rotate(v, cos, sin):
    return v * cos + pltpu.roll(v, v.shape[-1] // 2, 1) * sin


def pre_kernel(x_ref, gain_ref, wq_ref, wkv_ref, cos_ref, sin_ref, xn_ref, q_ref, kv_ref, *, scale):
    nb, seq, d_model = x_ref.shape
    hd = cos_ref.shape[1]
    rows = nb * seq
    x = x_ref[...].reshape(rows, d_model).astype(F32)
    inv = lax.rsqrt(jnp.mean(x * x, axis=-1, keepdims=True) + NORM_EPS)
    xn_ref[...] = (x * inv * (1.0 + gain_ref[...])).astype(BF16).reshape(nb, seq, d_model)
    xn = xn_ref[...].reshape(rows, d_model)
    cos = jnp.concatenate([cos_ref[...]] * nb, axis=0)
    sin = jnp.concatenate([sin_ref[...]] * nb, axis=0)
    kv = mm(xn, wkv_ref[...])
    kv_ref[:, :, :hd] = rotate(kv[:, :hd], cos, sin).astype(BF16).reshape(nb, seq, hd)
    kv_ref[:, :, hd:] = kv[:, hd:].astype(BF16).reshape(nb, seq, hd)
    width = wq_ref.shape[1]
    step = 512
    for n in range(width // step):
        proj = mm(xn, wq_ref[:, n * step:(n + 1) * step])
        for h in range(step // hd):
            rot = rotate(proj[:, h * hd:(h + 1) * hd], cos, sin) * scale
            lo = n * step + h * hd
            q_ref[:, :, lo:lo + hd] = rot.astype(BF16).reshape(nb, seq, hd)


def attention_kernel(batch, prefix_ref, q_ref, do_ref, kv_ref, cos_ref, sin_ref, o_ref, dq_ref, dkv_ref,
                     s_scr, e_scr, dp_scr, k_ext, v_scr, k_t, v_t, eye_scr, top_scr, stat_scr,
                     part, recv1, sum1, recv2, sum2, recv3,
                     send1, got1, send2, got2, send3, got3, free1, free2, free3, *, scale):
    t = pl.program_id(0)
    me = lax.axis_index('sp')
    core = me % 2
    x_bit = (me // 2) % 2
    y_bit = me // 4
    partner = me + 1 - 2 * core
    x_near = me + 2 - 4 * x_bit
    y_near = me + 4 - 8 * y_bit
    near_1 = x_near * (1 - core) + y_near * core
    near_2 = y_near * (1 - core) + x_near * core
    bit_1 = x_bit * (1 - core) + y_bit * core
    bit_2 = y_bit * (1 - core) + x_bit * core

    groups, _, seq, _ = kv_ref.shape
    hd = kv_ref.shape[3] // 2
    keys = groups * seq
    pairs = q_ref.shape[2] // (2 * hd)
    chunk = 256

    def copy_1(slot):
        return pltpu.make_async_remote_copy(part.at[slot, 1 - core], recv1.at[slot], send1.at[slot], got1.at[slot],
                                            device_id=(partner,), device_id_type=MESH)

    def copy_2(slot):
        return pltpu.make_async_remote_copy(sum1.at[slot, 1 - bit_1], recv2.at[slot], send2.at[slot], got2.at[slot],
                                            device_id=(near_1,), device_id_type=MESH)

    def copy_3(slot):
        return pltpu.make_async_remote_copy(sum2.at[slot, 1 - bit_2], recv3.at[slot], send3.at[slot], got3.at[slot],
                                            device_id=(near_2,), device_id_type=MESH)

    @pl.when(t == 0)
    def _():
        barrier = pltpu.get_barrier_semaphore()
        for other in (partner, near_1, near_2):
            pl.semaphore_signal(barrier, inc=1, device_id=(other,), device_id_type=MESH)
        pl.semaphore_wait(barrier, 3)

    @pl.when(t == 0)
    def _():
        eye_scr[...] = (lax.broadcasted_iota(jnp.int32, (seq, seq), 0)
                        == lax.broadcasted_iota(jnp.int32, (seq, seq), 1)).astype(F32).astype(BF16)

    def fold(a, op):
        return op(a.reshape(chunk // 8, 8, 2 * hd), axis=0)

    def heads_of(ref, lo):
        return jnp.concatenate([ref[0, :, pl.ds(lo, hd)], ref[0, :, pl.ds(lo + hd, hd)]], axis=0)

    def masked_q(lo):
        eye = eye_scr[...]
        return jnp.concatenate([heads_of(q_ref, lo), jnp.concatenate([eye, eye], axis=0)], axis=1)

    low = functools.partial(jnp.full, (8, 2 * hd), MASK_FILL, F32)

    @pl.when(t < batch)
    def _():
        slot = t % 2
        k_all = kv_ref[:, 0, :, :hd].reshape(keys, hd)
        v_all = kv_ref[:, 0, :, hd:].reshape(keys, hd)
        limit = jnp.maximum(prefix_ref[0, 0:1, :], me * seq + lax.broadcasted_iota(jnp.int32, (keys, seq), 1) + 1)
        k_ext[:, :hd] = k_all
        k_ext[:, hd:] = jnp.where(lax.broadcasted_iota(jnp.int32, (keys, seq), 0) < limit, 0.0, MASK_FILL).astype(BF16)
        v_scr[...] = v_all
        k_t[...] = k_all.T
        v_t[...] = v_all.T
        part[slot] = jnp.zeros(part.shape[1:], F32)

        def at_pair(i):
            return pl.multiple_of(i * 2 * hd, 2 * hd) if not isinstance(i, int) else i * 2 * hd

        def score_step(i, buf):
            q_ext = masked_q(at_pair(i))
            top = low()
            for c in range(keys // chunk):
                at = slice(c * chunk, (c + 1) * chunk)
                s = mm_nt(k_ext[at, :], q_ext)
                s_scr[buf, at, :] = s
                top = jnp.maximum(top, fold(s, jnp.max))
            top_scr[buf] = top

        def weigh_step(i, buf):
            do2 = heads_of(do_ref, at_pair(i))
            top = jnp.max(top_scr[buf], axis=0, keepdims=True)
            total = jnp.zeros((8, 2 * hd), F32)
            cross = jnp.zeros((8, 2 * hd), F32)
            for c in range(keys // chunk):
                at = slice(c * chunk, (c + 1) * chunk)
                dp = mm_nt(v_scr[at, :], do2).astype(BF16).astype(F32)
                e = jnp.exp(s_scr[buf, at, :] - top)
                e_scr[buf, at, :] = e
                dp_scr[buf, at, :] = dp
                total = total + fold(e, jnp.sum)
                cross = cross + fold(e * dp, jnp.sum)
            inv = 1.0 / jnp.sum(total, axis=0, keepdims=True)
            stat_scr[buf, 0:1, :] = inv
            stat_scr[buf, 1:2, :] = jnp.sum(cross, axis=0, keepdims=True) * inv

        def grad_step(i, buf):
            lo = at_pair(i)
            q2 = heads_of(q_ref, lo)
            do2 = heads_of(do_ref, lo)
            inv = stat_scr[buf, 0:1, :]
            delta = stat_scr[buf, 1:2, :]
            ps, dss = [], []
            for c in range(keys // chunk):
                at = slice(c * chunk, (c + 1) * chunk)
                p = e_scr[buf, at, :] * inv
                ds = (p * (dp_scr[buf, at, :] - delta)).astype(BF16)
                p = p.astype(BF16)
                ps.append(p)
                dss.append(ds)
                dk = mm(ds, q2)
                dv = mm(p, do2)
                for r in range(chunk // seq):
                    j = c * (chunk // seq) + r
                    part[slot, j % 2, j // 2, 0] += dk[r * seq:(r + 1) * seq, :]
                    part[slot, j % 2, j // 2, 1] += dv[r * seq:(r + 1) * seq, :]
            o_t = mm(v_t[...], jnp.concatenate(ps, axis=0)).astype(BF16)
            dq_t = mm(k_t[...], jnp.concatenate(dss, axis=0)).astype(BF16)
            for half in range(2):
                o_ref[0, :, pl.ds(lo + half * hd, hd)] = o_t[:, half * hd:(half + 1) * hd].T
                dq = dq_t[:, half * hd:(half + 1) * hd].T.astype(F32) * scale
                dq_ref[0, :, pl.ds(lo + half * hd, hd)] = rotate(dq, cos_ref[...], -sin_ref[...]).astype(BF16)

        def two_pairs(r, carry):
            i = 2 * r + 1
            score_step(i + 1, 0)
            weigh_step(i, 1)
            grad_step(i - 1, 0)
            score_step(i + 2, 1)
            weigh_step(i + 1, 0)
            grad_step(i, 1)
            return carry

        score_step(0, 0)
        score_step(1, 1)
        weigh_step(0, 0)
        lax.fori_loop(0, pairs // 2 - 1, two_pairs, 0)
        weigh_step(pairs - 1, 1)
        grad_step(pairs - 2, 0)
        grad_step(pairs - 1, 1)

    @pl.when(t >= 3)
    def _():
        slot = (t - 3) % 2
        copy_3(slot).wait()
        done = sum2[slot, bit_2] + recv3[slot]
        dkv_ref[0, :, :hd] = done[0]
        dkv_ref[0, :, hd:] = done[1]

        @pl.when(t - 3 < batch - 2)
        def _():
            pl.semaphore_signal(free3.at[slot], inc=1, device_id=(near_2,), device_id_type=MESH)

    @pl.when((t >= 2) & (t - 2 < batch))
    def _():
        slot = t % 2
        copy_2(slot).wait()
        for s in range(2):
            sum2[slot, s] = sum1[slot, bit_1, s] + recv2[slot, s]

        @pl.when(t - 2 < batch - 2)
        def _():
            pl.semaphore_signal(free2.at[slot], inc=1, device_id=(near_1,), device_id_type=MESH)

        @pl.when(t - 2 >= 2)
        def _():
            pl.semaphore_wait(free3.at[slot], 1)

        copy_3(slot).start()

    @pl.when((t >= 1) & (t - 1 < batch))
    def _():
        slot = (t - 1) % 2
        copy_1(slot).wait()
        for f in range(2):
            for s in range(2):
                chip = f * (1 + core) + s * (2 - core)
                sum1[slot, f, s] = part[slot, core, chip] + recv1[slot, chip]

        @pl.when(t - 1 < batch - 2)
        def _():
            pl.semaphore_signal(free1.at[slot], inc=1, device_id=(partner,), device_id_type=MESH)

        @pl.when(t - 1 >= 2)
        def _():
            pl.semaphore_wait(free2.at[slot], 1)

        copy_2(slot).start()

    @pl.when(t < batch)
    def _():
        slot = t % 2

        @pl.when(t >= 2)
        def _():
            pl.semaphore_wait(free1.at[slot], 1)

        copy_1(slot).start()


def post_kernel(dq_ref, dkv_ref, wq_ref, wkv_ref, x_ref, dy_ref, gain_ref, dx_ref, dgain_ref):
    nb, seq, d_model = x_ref.shape
    rows = nb * seq
    acc = mm_nt(dq_ref[...].reshape(rows, dq_ref.shape[2]), wq_ref[...])
    acc = acc + mm_nt(dkv_ref[...].reshape(rows, dkv_ref.shape[2]), wkv_ref[...])
    g = acc.astype(BF16).astype(F32)
    x = x_ref[...].reshape(rows, d_model).astype(F32)
    inv = lax.rsqrt(jnp.mean(x * x, axis=-1, keepdims=True) + NORM_EPS)
    xr = x * inv
    part = jnp.sum((g * xr).reshape(rows // 8, 8, d_model), axis=0)
    u = g * (1.0 + gain_ref[...])
    mean = jnp.mean(u * xr, axis=-1, keepdims=True)
    dy = dy_ref[...].reshape(rows, d_model).astype(F32)
    dx_ref[...] = (dy + inv * (u - xr * mean)).astype(BF16).reshape(nb, seq, d_model)

    @pl.when(pl.program_id(0) == 0)
    def _():
        dgain_ref[...] = jnp.zeros_like(dgain_ref)

    dgain_ref[...] += part


def solution(mesh):
    groups = mesh.shape['sp']
    seq_spec = P(None, 'sp', None)
    whole = P()

    def local_block(x, dy, prefix_len, w_norm, w_q, w_k, w_v, w_o):
        batch, seq, d_model = x.shape
        hd = w_k.shape[1]
        width = w_q.shape[1]
        keys = seq * groups
        tokens = batch * seq
        scale = hd ** -0.5
        me = lax.axis_index('sp')
        half = hd // 2
        freq = ROPE_THETA ** (-2.0 * jnp.arange(half, dtype=F32) / hd)
        angles = (me * seq + jnp.arange(seq)).astype(F32)[:, None] * freq[None, :]
        cos, sin = jnp.cos(angles), jnp.sin(angles)
        cos2 = jnp.concatenate([cos, cos], axis=1)
        sin2 = jnp.concatenate([-sin, sin], axis=1)
        gain = w_norm.astype(F32).reshape(1, d_model)
        w_kv = jnp.concatenate([w_k, w_v], axis=1)

        nb = 4

        def rows_spec(n, w):
            return pl.BlockSpec((n, seq, w), lambda i: (i, 0, 0))

        def full(*shape):
            return pl.BlockSpec(shape, lambda i: (0,) * len(shape))

        xn, q, kv = pl.pallas_call(
            functools.partial(pre_kernel, scale=scale),
            grid=(batch // nb,),
            in_specs=[rows_spec(nb, d_model), full(1, d_model), full(d_model, width), full(d_model, 2 * hd),
                      full(seq, hd), full(seq, hd)],
            out_specs=[rows_spec(nb, d_model), rows_spec(nb, width), rows_spec(nb, 2 * hd)],
            out_shape=[jax.ShapeDtypeStruct((batch, seq, d_model), BF16),
                       jax.ShapeDtypeStruct((batch, seq, width), BF16),
                       jax.ShapeDtypeStruct((batch, seq, 2 * hd), BF16)],
            compiler_params=pltpu.CompilerParams(vmem_limit_bytes=VMEM_LIMIT),
            cost_estimate=pl.CostEstimate(flops=2 * tokens * d_model * (width + 2 * hd),
                                          bytes_accessed=6 * tokens * d_model, transcendentals=0),
            name='project',
        )(x, gain, w_q, w_kv, cos2, sin2)

        kv_all = lax.all_gather(kv, 'sp', axis=0, tiled=False)
        d_o = jnp.einsum('bsd,ed->bse', dy, w_o, preferred_element_type=F32).astype(BF16)

        last = batch - 1
        steps = batch + 3
        f32_tile = (seq, hd)
        o, dq, dkv = pl.pallas_call(
            functools.partial(attention_kernel, batch, scale=scale),
            grid=(steps,),
            in_specs=[pl.BlockSpec((1, 8, hd), lambda i: (jnp.minimum(i, last), 0, 0)),
                      pl.BlockSpec((1, seq, width), lambda i: (jnp.minimum(i, last), 0, 0)),
                      pl.BlockSpec((1, seq, width), lambda i: (jnp.minimum(i, last), 0, 0)),
                      pl.BlockSpec((groups, 1, seq, 2 * hd), lambda i: (0, jnp.minimum(i, last), 0, 0)),
                      full(seq, hd), full(seq, hd)],
            out_specs=[pl.BlockSpec((1, seq, width), lambda i: (jnp.minimum(i, last), 0, 0)),
                       pl.BlockSpec((1, seq, width), lambda i: (jnp.minimum(i, last), 0, 0)),
                       pl.BlockSpec((1, seq, 2 * hd), lambda i: (jnp.maximum(i - 3, 0), 0, 0))],
            out_shape=[jax.ShapeDtypeStruct((batch, seq, width), BF16),
                       jax.ShapeDtypeStruct((batch, seq, width), BF16),
                       jax.ShapeDtypeStruct((batch, seq, 2 * hd), F32)],
            scratch_shapes=[
                pltpu.VMEM((2, keys, 2 * hd), F32), pltpu.VMEM((2, keys, 2 * hd), F32), pltpu.VMEM((2, keys, 2 * hd), F32),
                pltpu.VMEM((keys, 2 * hd), BF16), pltpu.VMEM((keys, hd), BF16),
                pltpu.VMEM((hd, keys), BF16), pltpu.VMEM((hd, keys), BF16),
                pltpu.VMEM((seq, seq), BF16), pltpu.VMEM((2, 8, 2 * hd), F32), pltpu.VMEM((2, 8, 2 * hd), F32),
                pltpu.VMEM((2, 2, 4, 2) + f32_tile, F32), pltpu.VMEM((2, 4, 2) + f32_tile, F32),
                pltpu.VMEM((2, 2, 2, 2) + f32_tile, F32), pltpu.VMEM((2, 2, 2) + f32_tile, F32),
                pltpu.VMEM((2, 2, 2) + f32_tile, F32), pltpu.VMEM((2, 2) + f32_tile, F32),
            ] + [pltpu.SemaphoreType.DMA((2,))] * 6 + [pltpu.SemaphoreType.REGULAR((2,))] * 3,
            compiler_params=pltpu.CompilerParams(vmem_limit_bytes=VMEM_LIMIT, collective_id=0, has_side_effects=True),
            cost_estimate=pl.CostEstimate(flops=12 * tokens * width * keys, bytes_accessed=12 * tokens * width,
                                          transcendentals=tokens * width // hd * keys),
            name='attend',
        )(jnp.broadcast_to(prefix_len[:, None, None], (batch, 8, hd)), q, d_o, kv_all, cos2, sin2)

        d_wo = jnp.einsum('bse,bsd->ed', o, dy, preferred_element_type=F32)
        d_wo, xn = lax.optimization_barrier((d_wo, xn))
        d_wo = lax.psum(d_wo, 'sp', axis_index_groups=[[m ^ 1 for m in range(groups)]])

        rot = dkv[..., :hd].astype(BF16).astype(F32)
        rolled = jnp.concatenate([rot[..., half:], rot[..., :half]], axis=-1)
        dk_proj = (rot * cos2 - rolled * sin2).astype(BF16)
        dkv_proj = jnp.concatenate([dk_proj, dkv[..., hd:].astype(BF16)], axis=-1)
        d_wq = jnp.einsum('bsd,bse->de', xn, dq, preferred_element_type=F32)
        d_wkv = jnp.einsum('bsd,bse->de', xn, dkv_proj, preferred_element_type=F32)
        d_wq, d_wkv, o, dq = lax.optimization_barrier((d_wq, d_wkv, o, dq))
        d_wq, d_wkv = lax.psum((d_wq, d_wkv), 'sp')

        mixed = jnp.einsum('bse,ed->bsd', o, w_o, preferred_element_type=F32)
        y = (x.astype(F32) + mixed).astype(BF16)

        nb2 = 2
        dx, dgain = pl.pallas_call(
            post_kernel,
            grid=(batch // nb2,),
            in_specs=[rows_spec(nb2, width), rows_spec(nb2, 2 * hd), full(d_model, width), full(d_model, 2 * hd),
                      rows_spec(nb2, d_model), rows_spec(nb2, d_model), full(1, d_model)],
            out_specs=[rows_spec(nb2, d_model), full(8, d_model)],
            out_shape=[jax.ShapeDtypeStruct((batch, seq, d_model), BF16), jax.ShapeDtypeStruct((8, d_model), F32)],
            compiler_params=pltpu.CompilerParams(vmem_limit_bytes=VMEM_LIMIT),
            cost_estimate=pl.CostEstimate(flops=2 * tokens * d_model * (width + 2 * hd),
                                          bytes_accessed=8 * tokens * d_model, transcendentals=0),
            name='norm_grad',
        )(dq, dkv_proj, w_q, w_kv, x, dy, gain)
        d_gain = lax.psum(jnp.sum(dgain, axis=0), 'sp')
        return y, dx, d_wq, d_wkv[:, :hd], d_wkv[:, hd:], d_wo, d_gain

    return jax.shard_map(local_block, mesh=mesh, in_specs=(seq_spec, seq_spec, whole, whole, whole, whole, whole, whole), out_specs=(seq_spec, seq_spec, whole, whole, whole, whole, whole), check_vma=False)
```

```python
import functools

import jax
import jax.numpy as jnp
from jax import lax
from jax.experimental import pallas as pl
from jax.experimental.pallas import tpu as pltpu
from jax.sharding import PartitionSpec as P


ROPE_THETA = 10000.0
NORM_EPS = 1e-6
MASK_FILL = -1e30
F32 = jnp.float32
BF16 = jnp.bfloat16
MESH = pl.DeviceIdType.MESH
CHUNKS = 4
VMEM_LIMIT = 60 * 1024 * 1024
NT = (((1,), (1,)), ((), ()))


def mm(a, b):
    return jnp.dot(a, b, preferred_element_type=F32)


def mm_nt(a, b):
    return lax.dot_general(a, b, NT, preferred_element_type=F32)


def rotate(v, cos, sin):
    return v * cos + pltpu.roll(v, v.shape[-1] // 2, 1) * sin


def norm_kernel(x_ref, gain_ref, wkv_ref, cos_ref, sin_ref, xn_ref, kv_ref):
    nb, seq, d_model = x_ref.shape
    hd = cos_ref.shape[1]
    rows = nb * seq
    x = x_ref[...].reshape(rows, d_model).astype(F32)
    inv = lax.rsqrt(jnp.mean(x * x, axis=-1, keepdims=True) + NORM_EPS)
    xn = (x * inv * (1.0 + gain_ref[...])).astype(BF16)
    xn_ref[...] = xn.reshape(nb, seq, d_model)
    cos = jnp.concatenate([cos_ref[...]] * nb, axis=0)
    sin = jnp.concatenate([sin_ref[...]] * nb, axis=0)
    kv = mm(xn, wkv_ref[...])
    kv_ref[:, :, :hd] = rotate(kv[:, :hd], cos, sin).astype(BF16).reshape(nb, seq, hd)
    kv_ref[:, :, hd:] = kv[:, hd:].astype(BF16).reshape(nb, seq, hd)


def query_kernel(xn_ref, wq_ref, cos_ref, sin_ref, q_ref, *, scale):
    nb, seq, d_model = xn_ref.shape
    hd = cos_ref.shape[1]
    xn = xn_ref[...].reshape(nb * seq, d_model)
    cos = jnp.concatenate([cos_ref[...]] * nb, axis=0)
    sin = jnp.concatenate([sin_ref[...]] * nb, axis=0)
    width = wq_ref.shape[1]
    step = 512
    for n in range(width // step):
        proj = mm(xn, wq_ref[:, n * step:(n + 1) * step])
        for h in range(step // hd):
            rot = rotate(proj[:, h * hd:(h + 1) * hd], cos, sin) * scale
            lo = n * step + h * hd
            q_ref[:, :, lo:lo + hd] = rot.astype(BF16).reshape(nb, seq, hd)


def attention_kernel(batch, first, last, *refs, scale):
    refs = list(refs)
    prefix_ref, q_ref, do_ref, q_was, do_was, kv_ref, cos_ref, sin_ref = refs[:8]
    del refs[:8]
    carry_ref = None if first else refs.pop(0)
    o_ref, dq_ref, dkv_ref = refs[:3]
    s_scr, e_scr, dp_scr, k_ext, v_scr, k_t, v_t, eye_scr, top_scr, stat_scr = refs[3:13]
    if last:
        (part, recv1, sum1, recv2, sum2, recv3,
         send1, got1, send2, got2, send3, got3, free1, free2, free3) = refs[13:]
    t = pl.program_id(0)
    me = lax.axis_index('sp')
    core = me % 2
    x_bit = (me // 2) % 2
    y_bit = me // 4
    partner = me + 1 - 2 * core
    x_near = me + 2 - 4 * x_bit
    y_near = me + 4 - 8 * y_bit
    near_1 = x_near * (1 - core) + y_near * core
    near_2 = y_near * (1 - core) + x_near * core
    bit_1 = x_bit * (1 - core) + y_bit * core
    bit_2 = y_bit * (1 - core) + x_bit * core

    groups, _, seq, _ = kv_ref.shape
    hd = kv_ref.shape[3] // 2
    keys = groups * seq
    chunk = 256

    def copy_1(slot):
        return pltpu.make_async_remote_copy(part.at[slot, 1 - core], recv1.at[slot], send1.at[slot], got1.at[slot],
                                            device_id=(partner,), device_id_type=MESH)

    def copy_2(slot):
        return pltpu.make_async_remote_copy(sum1.at[slot, 1 - bit_1], recv2.at[slot], send2.at[slot], got2.at[slot],
                                            device_id=(near_1,), device_id_type=MESH)

    def copy_3(slot):
        return pltpu.make_async_remote_copy(sum2.at[slot, 1 - bit_2], recv3.at[slot], send3.at[slot], got3.at[slot],
                                            device_id=(near_2,), device_id_type=MESH)

    if last:
        @pl.when(t == 0)
        def _():
            barrier = pltpu.get_barrier_semaphore()
            for other in (partner, near_1, near_2):
                pl.semaphore_signal(barrier, inc=1, device_id=(other,), device_id_type=MESH)
            pl.semaphore_wait(barrier, 3)

    @pl.when(t == 0)
    def _():
        eye_scr[...] = (lax.broadcasted_iota(jnp.int32, (seq, seq), 0)
                        == lax.broadcasted_iota(jnp.int32, (seq, seq), 1)).astype(F32).astype(BF16)

    def fold(a, op):
        return op(a.reshape(chunk // 8, 8, 2 * hd), axis=0)

    def heads_of(ref, lo):
        return jnp.concatenate([ref[0, :, pl.ds(lo, hd)], ref[0, :, pl.ds(lo + hd, hd)]], axis=0)

    def masked_q(lo):
        eye = eye_scr[...]
        return jnp.concatenate([heads_of(q_ref, lo), jnp.concatenate([eye, eye], axis=0)], axis=1)

    low = functools.partial(jnp.full, (8, 2 * hd), MASK_FILL, F32)

    @pl.when(t <= batch)
    def _():
        now, was = t % 2, (t + 1) % 2
        k_all = kv_ref[:, 0, :, :hd].reshape(keys, hd)
        v_all = kv_ref[:, 0, :, hd:].reshape(keys, hd)
        limit = jnp.maximum(prefix_ref[0, 0:1, :], me * seq + lax.broadcasted_iota(jnp.int32, (keys, seq), 1) + 1)
        k_ext[:, :hd] = k_all
        k_ext[:, hd:] = jnp.where(lax.broadcasted_iota(jnp.int32, (keys, seq), 0) < limit, 0.0, MASK_FILL).astype(BF16)
        v_scr[now] = v_all
        k_t[now] = k_all.T
        v_t[now] = v_all.T
        acc = part.at[was] if last else dkv_ref.at[0]
        acc[...] = jnp.zeros(acc.shape, F32) if first else carry_ref[0]

        def score_step(i):
            buf = i
            q_ext = masked_q(i * 2 * hd)
            top = low()
            for c in range(keys // chunk):
                at = slice(c * chunk, (c + 1) * chunk)
                s = mm_nt(k_ext[at, :], q_ext)
                s_scr[buf, at, :] = s
                top = jnp.maximum(top, fold(s, jnp.max))
            top_scr[buf] = top

        def weigh_step(i, source, v_slot):
            buf = i
            do2 = heads_of(source, i * 2 * hd)
            top = jnp.max(top_scr[buf], axis=0, keepdims=True)
            total = jnp.zeros((8, 2 * hd), F32)
            cross = jnp.zeros((8, 2 * hd), F32)
            for c in range(keys // chunk):
                at = slice(c * chunk, (c + 1) * chunk)
                dp = mm_nt(v_scr[v_slot, at, :], do2).astype(BF16).astype(F32)
                e = jnp.exp(s_scr[buf, at, :] - top)
                e_scr[buf, at, :] = e
                dp_scr[buf, at, :] = dp
                total = total + fold(e, jnp.sum)
                cross = cross + fold(e * dp, jnp.sum)
            inv = 1.0 / jnp.sum(total, axis=0, keepdims=True)
            stat_scr[buf, 0:1, :] = inv
            stat_scr[buf, 1:2, :] = jnp.sum(cross, axis=0, keepdims=True) * inv

        def grad_step(i):
            buf = i
            lo = i * 2 * hd
            q2 = heads_of(q_was, lo)
            do2 = heads_of(do_was, lo)
            inv = stat_scr[buf, 0:1, :]
            delta = stat_scr[buf, 1:2, :]
            ps, dss = [], []
            for c in range(keys // chunk):
                at = slice(c * chunk, (c + 1) * chunk)
                p = e_scr[buf, at, :] * inv
                ds = (p * (dp_scr[buf, at, :] - delta)).astype(BF16)
                p = p.astype(BF16)
                ps.append(p)
                dss.append(ds)
                dk = mm(ds, q2)
                dv = mm(p, do2)
                for r in range(chunk // seq):
                    j = c * (chunk // seq) + r
                    acc[j % 2, j // 2, 0] += dk[r * seq:(r + 1) * seq, :]
                    acc[j % 2, j // 2, 1] += dv[r * seq:(r + 1) * seq, :]
            o_t = mm(v_t[was], jnp.concatenate(ps, axis=0)).astype(BF16)
            dq_t = mm(k_t[was], jnp.concatenate(dss, axis=0)).astype(BF16)
            for half in range(2):
                o_ref[0, :, pl.ds(lo + half * hd, hd)] = o_t[:, half * hd:(half + 1) * hd].T
                dq = dq_t[:, half * hd:(half + 1) * hd].T.astype(F32) * scale
                dq_ref[0, :, pl.ds(lo + half * hd, hd)] = rotate(dq, cos_ref[...], -sin_ref[...]).astype(BF16)

        score_step(0)
        weigh_step(1, do_was, was)
        grad_step(0)
        score_step(1)
        weigh_step(0, do_ref, now)
        grad_step(1)

    if not last:
        return

    @pl.when(t >= 4)
    def _():
        slot = t % 2
        copy_3(slot).wait()
        done = sum2[slot, bit_2] + recv3[slot]
        dkv_ref[0, :, :hd] = done[0]
        dkv_ref[0, :, hd:] = done[1]

        @pl.when(t - 4 < batch - 2)
        def _():
            pl.semaphore_signal(free3.at[slot], inc=1, device_id=(near_2,), device_id_type=MESH)

    @pl.when((t >= 3) & (t - 3 < batch))
    def _():
        slot = (t + 1) % 2
        copy_2(slot).wait()
        for s in range(2):
            sum2[slot, s] = sum1[slot, bit_1, s] + recv2[slot, s]

        @pl.when(t - 3 < batch - 2)
        def _():
            pl.semaphore_signal(free2.at[slot], inc=1, device_id=(near_1,), device_id_type=MESH)

        @pl.when(t - 3 >= 2)
        def _():
            pl.semaphore_wait(free3.at[slot], 1)

        copy_3(slot).start()

    @pl.when((t >= 2) & (t - 2 < batch))
    def _():
        slot = t % 2
        copy_1(slot).wait()
        for f in range(2):
            for s in range(2):
                chip = f * (1 + core) + s * (2 - core)
                sum1[slot, f, s] = part[slot, core, chip] + recv1[slot, chip]

        @pl.when(t - 2 < batch - 2)
        def _():
            pl.semaphore_signal(free1.at[slot], inc=1, device_id=(partner,), device_id_type=MESH)

        @pl.when(t - 2 >= 2)
        def _():
            pl.semaphore_wait(free2.at[slot], 1)

        copy_2(slot).start()

    @pl.when((t >= 1) & (t - 1 < batch))
    def _():
        slot = (t + 1) % 2

        @pl.when(t - 1 >= 2)
        def _():
            pl.semaphore_wait(free1.at[slot], 1)

        copy_1(slot).start()


def out_kernel(*refs):
    *o_refs, wo_ref, x_ref, y_ref = refs
    nb, seq, d_model = x_ref.shape
    rows = nb * seq
    o = jnp.concatenate([r[...].reshape(rows, r.shape[2]) for r in o_refs], axis=1)
    step = 512
    for n in range(d_model // step):
        at = slice(n * step, (n + 1) * step)
        x = x_ref[:, :, at].reshape(rows, step).astype(F32)
        y_ref[:, :, at] = (x + mm(o, wo_ref[:, at])).astype(BF16).reshape(nb, seq, step)


def post_kernel(*refs):
    *dq_refs, dkv_ref, wq_ref, wkv_ref, x_ref, dy_ref, gain_ref, dx_ref, dgain_ref = refs
    nb, seq, d_model = x_ref.shape
    rows = nb * seq
    dq = jnp.concatenate([r[...].reshape(rows, r.shape[2]) for r in dq_refs], axis=1)
    acc = mm_nt(dq, wq_ref[...])
    acc = acc + mm_nt(dkv_ref[...].reshape(rows, dkv_ref.shape[2]), wkv_ref[...])
    g = acc.astype(BF16).astype(F32)
    x = x_ref[...].reshape(rows, d_model).astype(F32)
    inv = lax.rsqrt(jnp.mean(x * x, axis=-1, keepdims=True) + NORM_EPS)
    xr = x * inv
    part = jnp.sum((g * xr).reshape(rows // 8, 8, d_model), axis=0)
    u = g * (1.0 + gain_ref[...])
    mean = jnp.mean(u * xr, axis=-1, keepdims=True)
    dy = dy_ref[...].reshape(rows, d_model).astype(F32)
    dx_ref[...] = (dy + inv * (u - xr * mean)).astype(BF16).reshape(nb, seq, d_model)

    @pl.when(pl.program_id(0) == 0)
    def _():
        dgain_ref[...] = jnp.zeros_like(dgain_ref)

    dgain_ref[...] += part


def solution(mesh):
    groups = mesh.shape['sp']
    seq_spec = P(None, 'sp', None)
    whole = P()

    def local_block(x, dy, prefix_len, w_norm, w_q, w_k, w_v, w_o):
        batch, seq, d_model = x.shape
        hd = w_k.shape[1]
        width = w_q.shape[1]
        keys = seq * groups
        tokens = batch * seq
        scale = hd ** -0.5
        me = lax.axis_index('sp')
        half = hd // 2
        freq = ROPE_THETA ** (-2.0 * jnp.arange(half, dtype=F32) / hd)
        angles = (me * seq + jnp.arange(seq)).astype(F32)[:, None] * freq[None, :]
        cos, sin = jnp.cos(angles), jnp.sin(angles)
        cos2 = jnp.concatenate([cos, cos], axis=1)
        sin2 = jnp.concatenate([-sin, sin], axis=1)
        gain = w_norm.astype(F32).reshape(1, d_model)
        w_kv = jnp.concatenate([w_k, w_v], axis=1)

        nb = 4

        def rows_spec(n, w):
            return pl.BlockSpec((n, seq, w), lambda i: (i, 0, 0))

        def full(*shape):
            return pl.BlockSpec(shape, lambda i: (0,) * len(shape))

        xn, kv = pl.pallas_call(
            norm_kernel,
            grid=(batch // nb,),
            in_specs=[rows_spec(nb, d_model), full(1, d_model), full(d_model, 2 * hd), full(seq, hd), full(seq, hd)],
            out_specs=[rows_spec(nb, d_model), rows_spec(nb, 2 * hd)],
            out_shape=[jax.ShapeDtypeStruct((batch, seq, d_model), BF16),
                       jax.ShapeDtypeStruct((batch, seq, 2 * hd), BF16)],
            compiler_params=pltpu.CompilerParams(vmem_limit_bytes=VMEM_LIMIT),
            cost_estimate=pl.CostEstimate(flops=4 * tokens * d_model * hd, bytes_accessed=4 * tokens * d_model,
                                          transcendentals=0),
            name='norm',
        )(x, gain, w_kv, cos2, sin2)
        kv_all = lax.all_gather(kv, 'sp', axis=0, tiled=False)
        q = pl.pallas_call(
            functools.partial(query_kernel, scale=scale),
            grid=(batch // nb,),
            in_specs=[rows_spec(nb, d_model), full(d_model, width), full(seq, hd), full(seq, hd)],
            out_specs=rows_spec(nb, width),
            out_shape=jax.ShapeDtypeStruct((batch, seq, width), BF16),
            compiler_params=pltpu.CompilerParams(vmem_limit_bytes=VMEM_LIMIT),
            cost_estimate=pl.CostEstimate(flops=2 * tokens * d_model * width, bytes_accessed=4 * tokens * d_model,
                                          transcendentals=0),
            name='query',
        )(xn, w_q, cos2, sin2)
        d_o = jnp.einsum('bsd,ed->bse', dy, w_o, preferred_element_type=F32).astype(BF16)

        end = batch - 1
        f32_tile = (seq, hd)
        prefix = jnp.broadcast_to(prefix_len[:, None, None], (batch, 8, hd))
        cols = width // CHUNKS
        split = (2, groups // 2, 2) + f32_tile

        def attend(n, q, d_o, carry):
            first, last = n == 0, n == CHUNKS - 1
            before = lambda i: jnp.clip(i - 1, 0, end)
            here = lambda i: (before(i), 0, 0)
            part_spec = pl.BlockSpec((1,) + split, lambda i: (before(i), 0, 0, 0, 0, 0))
            in_specs = [pl.BlockSpec((1, 8, hd), lambda i: (jnp.minimum(i, end), 0, 0)),
                        pl.BlockSpec((1, seq, cols), lambda i: (jnp.minimum(i, end), 0, n)),
                        pl.BlockSpec((1, seq, cols), lambda i: (jnp.minimum(i, end), 0, n)),
                        pl.BlockSpec((1, seq, cols), lambda i: (before(i), 0, n)),
                        pl.BlockSpec((1, seq, cols), lambda i: (before(i), 0, n)),
                        pl.BlockSpec((groups, 1, seq, 2 * hd), lambda i: (0, jnp.minimum(i, end), 0, 0)),
                        full(seq, hd), full(seq, hd)]
            args = [prefix, q, d_o, q, d_o, kv_all, cos2, sin2]
            if not first:
                in_specs.append(part_spec)
                args.append(carry)
            scratch = [
                pltpu.VMEM((2, keys, 2 * hd), F32), pltpu.VMEM((2, keys, 2 * hd), F32), pltpu.VMEM((2, keys, 2 * hd), F32),
                pltpu.VMEM((keys, 2 * hd), BF16), pltpu.VMEM((2, keys, hd), BF16),
                pltpu.VMEM((2, hd, keys), BF16), pltpu.VMEM((2, hd, keys), BF16),
                pltpu.VMEM((seq, seq), BF16), pltpu.VMEM((2, 8, 2 * hd), F32), pltpu.VMEM((2, 8, 2 * hd), F32)]
            params = dict(vmem_limit_bytes=VMEM_LIMIT)
            if last:
                dkv_spec = pl.BlockSpec((1, seq, 2 * hd), lambda i: (jnp.maximum(i - 4, 0), 0, 0))
                dkv_shape = jax.ShapeDtypeStruct((batch, seq, 2 * hd), F32)
                scratch += [pltpu.VMEM((2,) + split, F32), pltpu.VMEM((2, 4, 2) + f32_tile, F32),
                            pltpu.VMEM((2, 2, 2, 2) + f32_tile, F32), pltpu.VMEM((2, 2, 2) + f32_tile, F32),
                            pltpu.VMEM((2, 2, 2) + f32_tile, F32), pltpu.VMEM((2, 2) + f32_tile, F32)]
                scratch += [pltpu.SemaphoreType.DMA((2,))] * 6 + [pltpu.SemaphoreType.REGULAR((2,))] * 3
                params.update(collective_id=0, has_side_effects=True)
            else:
                dkv_spec = part_spec
                dkv_shape = jax.ShapeDtypeStruct((batch,) + split, F32)
            return pl.pallas_call(
                functools.partial(attention_kernel, batch, first, last, scale=scale),
                grid=(batch + 1 + 3 * last,),
                in_specs=in_specs,
                out_specs=[pl.BlockSpec((1, seq, cols), here), pl.BlockSpec((1, seq, cols), here), dkv_spec],
                out_shape=[jax.ShapeDtypeStruct((batch, seq, cols), BF16),
                           jax.ShapeDtypeStruct((batch, seq, cols), BF16), dkv_shape],
                scratch_shapes=scratch,
                compiler_params=pltpu.CompilerParams(**params),
                cost_estimate=pl.CostEstimate(flops=12 * tokens * cols * keys, bytes_accessed=12 * tokens * cols,
                                              transcendentals=tokens * cols // hd * keys),
                name='attend',
            )(*args)

        os, dqs, d_wos, d_wqs = [], [], [], []
        carry = None
        for n in range(CHUNKS):
            o, dq, carry = attend(n, q, d_o, carry)
            os.append(o)
            dqs.append(dq)
            d_wo = jnp.einsum('bse,bsd->ed', o, dy, preferred_element_type=F32)
            d_wq = jnp.einsum('bsd,bse->de', xn, dq, preferred_element_type=F32)
            if n < CHUNKS - 1:
                d_wo, d_wq, q, carry = lax.optimization_barrier((d_wo, d_wq, q, carry))
                order = [m ^ (n + 1) for m in range(groups)]
                d_wo, d_wq = lax.psum((d_wo, d_wq), 'sp', axis_index_groups=[order])
            else:
                dkv = carry
                rot = dkv[..., :hd].astype(BF16).astype(F32)
                rolled = jnp.concatenate([rot[..., half:], rot[..., :half]], axis=-1)
                dk_proj = (rot * cos2 - rolled * sin2).astype(BF16)
                dkv_proj = jnp.concatenate([dk_proj, dkv[..., hd:].astype(BF16)], axis=-1)
                d_wkv = jnp.einsum('bsd,bse->de', xn, dkv_proj, preferred_element_type=F32)
                d_wo, d_wq, d_wkv, x_b, dy_b = lax.optimization_barrier((d_wo, d_wq, d_wkv, x, dy))
                d_wo, d_wq, d_wkv = lax.psum((d_wo, d_wq, d_wkv), 'sp')
            d_wos.append(d_wo)
            d_wqs.append(d_wq)
        d_wo = jnp.concatenate(d_wos, axis=0)
        d_wq = jnp.concatenate(d_wqs, axis=1)

        nb2 = 2
        dx, dgain = pl.pallas_call(
            post_kernel,
            grid=(batch // nb2,),
            in_specs=[rows_spec(nb2, cols)] * CHUNKS + [
                rows_spec(nb2, 2 * hd), full(d_model, width), full(d_model, 2 * hd),
                rows_spec(nb2, d_model), rows_spec(nb2, d_model), full(1, d_model)],
            out_specs=[rows_spec(nb2, d_model), full(8, d_model)],
            out_shape=[jax.ShapeDtypeStruct((batch, seq, d_model), BF16), jax.ShapeDtypeStruct((8, d_model), F32)],
            compiler_params=pltpu.CompilerParams(vmem_limit_bytes=VMEM_LIMIT),
            cost_estimate=pl.CostEstimate(flops=2 * tokens * d_model * (width + 2 * hd),
                                          bytes_accessed=8 * tokens * d_model, transcendentals=0),
            name='norm_grad',
        )(*dqs, dkv_proj, w_q, w_kv, x_b, dy_b, gain)
        d_gain = lax.psum(jnp.sum(dgain, axis=0), 'sp')
        y = pl.pallas_call(
            out_kernel,
            grid=(batch // nb,),
            in_specs=[rows_spec(nb, cols)] * CHUNKS + [full(width, d_model), rows_spec(nb, d_model)],
            out_specs=rows_spec(nb, d_model),
            out_shape=jax.ShapeDtypeStruct((batch, seq, d_model), BF16),
            compiler_params=pltpu.CompilerParams(vmem_limit_bytes=VMEM_LIMIT),
            cost_estimate=pl.CostEstimate(flops=2 * tokens * d_model * width, bytes_accessed=6 * tokens * d_model,
                                          transcendentals=0),
            name='output',
        )(*os, w_o, x_b)
        return y, dx, d_wq, d_wkv[:, :hd], d_wkv[:, hd:], d_wo, d_gain


    return jax.shard_map(local_block, mesh=mesh, in_specs=(seq_spec, seq_spec, whole, whole, whole, whole, whole, whole), out_specs=(seq_spec, seq_spec, whole, whole, whole, whole, whole), check_vma=False)
```

```python
import functools

import jax
import jax.numpy as jnp
from jax import lax
from jax.experimental import pallas as pl
from jax.experimental.pallas import tpu as pltpu
from jax.sharding import PartitionSpec as P


ROPE_THETA = 10000.0
NORM_EPS = 1e-6
MASK_FILL = -1e30
F32 = jnp.float32
BF16 = jnp.bfloat16
MESH = pl.DeviceIdType.MESH
CHUNKS = 2
SUBS = 2
SLOTS = 3
LAG = 3
VMEM_LIMIT = 60 * 1024 * 1024
NT = (((1,), (1,)), ((), ()))


def mm(a, b):
    return jnp.dot(a, b, preferred_element_type=F32)


def mm_nt(a, b):
    return lax.dot_general(a, b, NT, preferred_element_type=F32)


def rotate(v, cos, sin):
    return v * cos + pltpu.roll(v, v.shape[-1] // 2, 1) * sin


def norm_kernel(x_ref, gain_ref, wkv_ref, cos_ref, sin_ref, xn_ref, kv_ref):
    nb, seq, d_model = x_ref.shape
    hd = cos_ref.shape[1]
    rows = nb * seq
    x = x_ref[...].reshape(rows, d_model).astype(F32)
    inv = lax.rsqrt(jnp.mean(x * x, axis=-1, keepdims=True) + NORM_EPS)
    xn = (x * inv * (1.0 + gain_ref[...])).astype(BF16)
    xn_ref[...] = xn.reshape(nb, seq, d_model)
    cos = jnp.concatenate([cos_ref[...]] * nb, axis=0)
    sin = jnp.concatenate([sin_ref[...]] * nb, axis=0)
    kv = mm(xn, wkv_ref[...])
    kv_ref[:, :, :hd] = rotate(kv[:, :hd], cos, sin).astype(BF16).reshape(nb, seq, hd)
    kv_ref[:, :, hd:] = kv[:, hd:].astype(BF16).reshape(nb, seq, hd)


def query_kernel(xn_ref, wq_ref, cos_ref, sin_ref, q_ref, *, scale):
    nb, seq, d_model = xn_ref.shape
    hd = cos_ref.shape[1]
    xn = xn_ref[...].reshape(nb * seq, d_model)
    cos = jnp.concatenate([cos_ref[...]] * nb, axis=0)
    sin = jnp.concatenate([sin_ref[...]] * nb, axis=0)
    width = wq_ref.shape[1]
    step = 512
    for n in range(width // step):
        proj = mm(xn, wq_ref[:, n * step:(n + 1) * step])
        for h in range(step // hd):
            rot = rotate(proj[:, h * hd:(h + 1) * hd], cos, sin) * scale
            lo = n * step + h * hd
            q_ref[:, :, lo:lo + hd] = rot.astype(BF16).reshape(nb, seq, hd)


def attention_kernel(batch, first, last, *refs, scale):
    refs = list(refs)
    prefix_ref, q_ref, do_ref, q_was, do_was, kv_ref, cos_ref, sin_ref = refs[:8]
    del refs[:8]
    carry_ref = None if first else refs.pop(0)
    o_ref, dq_ref, dkv_ref = refs[:3]
    s_scr, e_scr, dp_scr, k_ext, v_scr, k_t, v_t, eye_scr, top_scr, stat_scr = refs[3:13]
    if last:
        (part, recv1, sum1, recv2, sum2, recv3,
         send1, got1, send2, got2, send3, got3, free1, free2, free3) = refs[13:]
    t = pl.program_id(0)
    steps = SUBS * batch
    me = lax.axis_index('sp')
    core = me % 2
    x_bit = (me // 2) % 2
    y_bit = me // 4
    partner = me + 1 - 2 * core
    x_near = me + 2 - 4 * x_bit
    y_near = me + 4 - 8 * y_bit
    near_1 = x_near * (1 - core) + y_near * core
    near_2 = y_near * (1 - core) + x_near * core
    bit_1 = x_bit * (1 - core) + y_bit * core
    bit_2 = y_bit * (1 - core) + x_bit * core

    groups, _, seq, _ = kv_ref.shape
    hd = kv_ref.shape[3] // 2
    keys = groups * seq
    chunk = 256

    def copy_1(slot):
        return pltpu.make_async_remote_copy(part.at[slot, 1 - core], recv1.at[slot], send1.at[slot], got1.at[slot],
                                            device_id=(partner,), device_id_type=MESH)

    def copy_2(slot):
        return pltpu.make_async_remote_copy(sum1.at[slot, 1 - bit_1], recv2.at[slot], send2.at[slot], got2.at[slot],
                                            device_id=(near_1,), device_id_type=MESH)

    def copy_3(slot):
        return pltpu.make_async_remote_copy(sum2.at[slot, 1 - bit_2], recv3.at[slot], send3.at[slot], got3.at[slot],
                                            device_id=(near_2,), device_id_type=MESH)

    if last:
        @pl.when(t == 0)
        def _():
            barrier = pltpu.get_barrier_semaphore()
            for other in (partner, near_1, near_2):
                pl.semaphore_signal(barrier, inc=1, device_id=(other,), device_id_type=MESH)
            pl.semaphore_wait(barrier, 3)

    @pl.when(t == 0)
    def _():
        eye_scr[...] = (lax.broadcasted_iota(jnp.int32, (seq, seq), 0)
                        == lax.broadcasted_iota(jnp.int32, (seq, seq), 1)).astype(F32).astype(BF16)

    def fold(a, op):
        return op(a.reshape(chunk // 8, 8, 2 * hd), axis=0)

    def heads_of(ref, lo):
        return jnp.concatenate([ref[0, :, pl.ds(lo, hd)], ref[0, :, pl.ds(lo + hd, hd)]], axis=0)

    def masked_q(lo):
        eye = eye_scr[...]
        return jnp.concatenate([heads_of(q_ref, lo), jnp.concatenate([eye, eye], axis=0)], axis=1)

    low = functools.partial(jnp.full, (8, 2 * hd), MASK_FILL, F32)

    acc = part.at[((t + SUBS - 1) // SUBS + SLOTS - 1) % SLOTS] if last else dkv_ref.at[0]

    @pl.when((t % SUBS == 1 % SUBS) & (t <= steps))
    def _():
        acc[...] = jnp.zeros(acc.shape, F32) if first else carry_ref[0]

    @pl.when(t <= steps)
    def _():
        now, was = t % 2, (t + 1) % 2
        k_all = kv_ref[:, 0, :, :hd].reshape(keys, hd)
        v_all = kv_ref[:, 0, :, hd:].reshape(keys, hd)
        limit = jnp.maximum(prefix_ref[0, 0:1, :], me * seq + lax.broadcasted_iota(jnp.int32, (keys, seq), 1) + 1)
        k_ext[:, :hd] = k_all
        k_ext[:, hd:] = jnp.where(lax.broadcasted_iota(jnp.int32, (keys, seq), 0) < limit, 0.0, MASK_FILL).astype(BF16)
        v_scr[now] = v_all
        k_t[now] = k_all.T
        v_t[now] = v_all.T

        def score_step(i):
            buf = i
            q_ext = masked_q(i * 2 * hd)
            top = low()
            for c in range(keys // chunk):
                at = slice(c * chunk, (c + 1) * chunk)
                s = mm_nt(k_ext[at, :], q_ext)
                s_scr[buf, at, :] = s
                top = jnp.maximum(top, fold(s, jnp.max))
            top_scr[buf] = top

        def weigh_step(i, source, v_slot):
            buf = i
            do2 = heads_of(source, i * 2 * hd)
            top = jnp.max(top_scr[buf], axis=0, keepdims=True)
            total = jnp.zeros((8, 2 * hd), F32)
            cross = jnp.zeros((8, 2 * hd), F32)
            for c in range(keys // chunk):
                at = slice(c * chunk, (c + 1) * chunk)
                dp = mm_nt(v_scr[v_slot, at, :], do2).astype(BF16).astype(F32)
                e = jnp.exp(s_scr[buf, at, :] - top)
                e_scr[buf, at, :] = e
                dp_scr[buf, at, :] = dp
                total = total + fold(e, jnp.sum)
                cross = cross + fold(e * dp, jnp.sum)
            inv = 1.0 / jnp.sum(total, axis=0, keepdims=True)
            stat_scr[buf, 0:1, :] = inv
            stat_scr[buf, 1:2, :] = jnp.sum(cross, axis=0, keepdims=True) * inv

        def grad_step(i):
            buf = i
            lo = i * 2 * hd
            q2 = heads_of(q_was, lo)
            do2 = heads_of(do_was, lo)
            inv = stat_scr[buf, 0:1, :]
            delta = stat_scr[buf, 1:2, :]
            ps, dss = [], []
            for c in range(keys // chunk):
                at = slice(c * chunk, (c + 1) * chunk)
                p = e_scr[buf, at, :] * inv
                ds = (p * (dp_scr[buf, at, :] - delta)).astype(BF16)
                p = p.astype(BF16)
                ps.append(p)
                dss.append(ds)
                dk = mm(ds, q2)
                dv = mm(p, do2)
                for r in range(chunk // seq):
                    j = c * (chunk // seq) + r
                    acc[j % 2, j // 2, 0] += dk[r * seq:(r + 1) * seq, :]
                    acc[j % 2, j // 2, 1] += dv[r * seq:(r + 1) * seq, :]
            o_t = mm(v_t[was], jnp.concatenate(ps, axis=0)).astype(BF16)
            dq_t = mm(k_t[was], jnp.concatenate(dss, axis=0)).astype(BF16)
            for half in range(2):
                o_ref[0, :, pl.ds(lo + half * hd, hd)] = o_t[:, half * hd:(half + 1) * hd].T
                dq = dq_t[:, half * hd:(half + 1) * hd].T.astype(F32) * scale
                dq_ref[0, :, pl.ds(lo + half * hd, hd)] = rotate(dq, cos_ref[...], -sin_ref[...]).astype(BF16)

        score_step(0)
        weigh_step(1, do_was, was)
        grad_step(0)
        score_step(1)
        weigh_step(0, do_ref, now)
        grad_step(1)

    if not last:
        return

    def stage(number):
        ahead = t - LAG * number
        b = ahead // SUBS - 1
        return b, (ahead >= SUBS) & (ahead % SUBS == 0) & (b < batch)

    b4, due4 = stage(3)

    @pl.when(due4)
    def _():
        slot = b4 % SLOTS
        copy_3(slot).wait()
        done = sum2[slot, bit_2] + recv3[slot]
        dkv_ref[0, :, :hd] = done[0]
        dkv_ref[0, :, hd:] = done[1]

        @pl.when(b4 + SLOTS < batch)
        def _():
            pl.semaphore_signal(free3.at[slot], inc=1, device_id=(near_2,), device_id_type=MESH)

    b3, due3 = stage(2)

    @pl.when(due3)
    def _():
        slot = b3 % SLOTS
        copy_2(slot).wait()
        for s in range(2):
            sum2[slot, s] = sum1[slot, bit_1, s] + recv2[slot, s]

        @pl.when(b3 + SLOTS < batch)
        def _():
            pl.semaphore_signal(free2.at[slot], inc=1, device_id=(near_1,), device_id_type=MESH)

        @pl.when(b3 >= SLOTS)
        def _():
            pl.semaphore_wait(free3.at[slot], 1)

        copy_3(slot).start()

    b2, due2 = stage(1)

    @pl.when(due2)
    def _():
        slot = b2 % SLOTS
        copy_1(slot).wait()
        for f in range(2):
            for s in range(2):
                chip = f * (1 + core) + s * (2 - core)
                sum1[slot, f, s] = part[slot, core, chip] + recv1[slot, chip]

        @pl.when(b2 + SLOTS < batch)
        def _():
            pl.semaphore_signal(free1.at[slot], inc=1, device_id=(partner,), device_id_type=MESH)

        @pl.when(b2 >= SLOTS)
        def _():
            pl.semaphore_wait(free2.at[slot], 1)

        copy_2(slot).start()

    b1, due1 = stage(0)

    @pl.when(due1)
    def _():
        slot = b1 % SLOTS

        @pl.when(b1 >= SLOTS)
        def _():
            pl.semaphore_wait(free1.at[slot], 1)

        copy_1(slot).start()


def out_kernel(*refs):
    *o_refs, wo_ref, x_ref, y_ref = refs
    nb, seq, d_model = x_ref.shape
    rows = nb * seq
    o = jnp.concatenate([r[...].reshape(rows, r.shape[2]) for r in o_refs], axis=1)
    step = 512
    for n in range(d_model // step):
        at = slice(n * step, (n + 1) * step)
        x = x_ref[:, :, at].reshape(rows, step).astype(F32)
        y_ref[:, :, at] = (x + mm(o, wo_ref[:, at])).astype(BF16).reshape(nb, seq, step)


def post_kernel(*refs):
    *dq_refs, dkv_ref, wq_ref, wkv_ref, x_ref, dy_ref, gain_ref, dx_ref, dgain_ref = refs
    nb, seq, d_model = x_ref.shape
    rows = nb * seq
    dq = jnp.concatenate([r[...].reshape(rows, r.shape[2]) for r in dq_refs], axis=1)
    acc = mm_nt(dq, wq_ref[...])
    acc = acc + mm_nt(dkv_ref[...].reshape(rows, dkv_ref.shape[2]), wkv_ref[...])
    g = acc.astype(BF16).astype(F32)
    x = x_ref[...].reshape(rows, d_model).astype(F32)
    inv = lax.rsqrt(jnp.mean(x * x, axis=-1, keepdims=True) + NORM_EPS)
    xr = x * inv
    part = jnp.sum((g * xr).reshape(rows // 8, 8, d_model), axis=0)
    u = g * (1.0 + gain_ref[...])
    mean = jnp.mean(u * xr, axis=-1, keepdims=True)
    dy = dy_ref[...].reshape(rows, d_model).astype(F32)
    dx_ref[...] = (dy + inv * (u - xr * mean)).astype(BF16).reshape(nb, seq, d_model)

    @pl.when(pl.program_id(0) == 0)
    def _():
        dgain_ref[...] = jnp.zeros_like(dgain_ref)

    dgain_ref[...] += part


def solution(mesh):
    groups = mesh.shape['sp']
    seq_spec = P(None, 'sp', None)
    whole = P()

    def local_block(x, dy, prefix_len, w_norm, w_q, w_k, w_v, w_o):
        batch, seq, d_model = x.shape
        hd = w_k.shape[1]
        width = w_q.shape[1]
        keys = seq * groups
        tokens = batch * seq
        scale = hd ** -0.5
        me = lax.axis_index('sp')
        half = hd // 2
        freq = ROPE_THETA ** (-2.0 * jnp.arange(half, dtype=F32) / hd)
        angles = (me * seq + jnp.arange(seq)).astype(F32)[:, None] * freq[None, :]
        cos, sin = jnp.cos(angles), jnp.sin(angles)
        cos2 = jnp.concatenate([cos, cos], axis=1)
        sin2 = jnp.concatenate([-sin, sin], axis=1)
        gain = w_norm.astype(F32).reshape(1, d_model)
        w_kv = jnp.concatenate([w_k, w_v], axis=1)

        nb = 4

        def rows_spec(n, w):
            return pl.BlockSpec((n, seq, w), lambda i: (i, 0, 0))

        def full(*shape):
            return pl.BlockSpec(shape, lambda i: (0,) * len(shape))

        xn, kv = pl.pallas_call(
            norm_kernel,
            grid=(batch // nb,),
            in_specs=[rows_spec(nb, d_model), full(1, d_model), full(d_model, 2 * hd), full(seq, hd), full(seq, hd)],
            out_specs=[rows_spec(nb, d_model), rows_spec(nb, 2 * hd)],
            out_shape=[jax.ShapeDtypeStruct((batch, seq, d_model), BF16),
                       jax.ShapeDtypeStruct((batch, seq, 2 * hd), BF16)],
            compiler_params=pltpu.CompilerParams(vmem_limit_bytes=VMEM_LIMIT),
            cost_estimate=pl.CostEstimate(flops=4 * tokens * d_model * hd, bytes_accessed=4 * tokens * d_model,
                                          transcendentals=0),
            name='norm',
        )(x, gain, w_kv, cos2, sin2)
        kv_all = lax.all_gather(kv, 'sp', axis=0, tiled=False)
        q = pl.pallas_call(
            functools.partial(query_kernel, scale=scale),
            grid=(batch // nb,),
            in_specs=[rows_spec(nb, d_model), full(d_model, width), full(seq, hd), full(seq, hd)],
            out_specs=rows_spec(nb, width),
            out_shape=jax.ShapeDtypeStruct((batch, seq, width), BF16),
            compiler_params=pltpu.CompilerParams(vmem_limit_bytes=VMEM_LIMIT),
            cost_estimate=pl.CostEstimate(flops=2 * tokens * d_model * width, bytes_accessed=4 * tokens * d_model,
                                          transcendentals=0),
            name='query',
        )(xn, w_q, cos2, sin2)
        d_o = jnp.einsum('bsd,ed->bse', dy, w_o, preferred_element_type=F32).astype(BF16)

        f32_tile = (seq, hd)
        prefix = jnp.broadcast_to(prefix_len[:, None, None], (batch, 8, hd))
        cols = width // CHUNKS
        split = (2, groups // 2, 2) + f32_tile

        def attend(n, q, d_o, carry):
            first, last = n == 0, n == CHUNKS - 1
            top = SUBS * batch - 1
            now = lambda i: jnp.minimum(i, top)
            before = lambda i: jnp.clip(i - 1, 0, top)
            wide = cols // SUBS
            here = lambda i: (before(i) // SUBS, 0, before(i) % SUBS)
            part_spec = pl.BlockSpec((1,) + split, lambda i: (before(i) // SUBS, 0, 0, 0, 0, 0))
            at_now = pl.BlockSpec((1, seq, wide), lambda i: (now(i) // SUBS, 0, SUBS * n + now(i) % SUBS))
            at_before = pl.BlockSpec((1, seq, wide), lambda i: (before(i) // SUBS, 0, SUBS * n + before(i) % SUBS))
            in_specs = [pl.BlockSpec((1, 8, hd), lambda i: (now(i) // SUBS, 0, 0)),
                        at_now, at_now, at_before, at_before,
                        pl.BlockSpec((groups, 1, seq, 2 * hd), lambda i: (0, now(i) // SUBS, 0, 0)),
                        full(seq, hd), full(seq, hd)]
            args = [prefix, q, d_o, q, d_o, kv_all, cos2, sin2]
            if not first:
                in_specs.append(part_spec)
                args.append(carry)
            scratch = [
                pltpu.VMEM((2, keys, 2 * hd), F32), pltpu.VMEM((2, keys, 2 * hd), F32), pltpu.VMEM((2, keys, 2 * hd), F32),
                pltpu.VMEM((keys, 2 * hd), BF16), pltpu.VMEM((2, keys, hd), BF16),
                pltpu.VMEM((2, hd, keys), BF16), pltpu.VMEM((2, hd, keys), BF16),
                pltpu.VMEM((seq, seq), BF16), pltpu.VMEM((2, 8, 2 * hd), F32), pltpu.VMEM((2, 8, 2 * hd), F32)]
            params = dict(vmem_limit_bytes=VMEM_LIMIT)
            if last:
                dkv_spec = pl.BlockSpec((1, seq, 2 * hd), lambda i: (jnp.maximum(i - SUBS - 3 * LAG, 0) // SUBS, 0, 0))
                dkv_shape = jax.ShapeDtypeStruct((batch, seq, 2 * hd), F32)
                scratch += [pltpu.VMEM((SLOTS,) + shape + f32_tile, F32) for shape in
                            ((2, groups // 2, 2), (4, 2), (2, 2, 2), (2, 2), (2, 2), (2,))]
                scratch += [pltpu.SemaphoreType.DMA((SLOTS,))] * 6 + [pltpu.SemaphoreType.REGULAR((SLOTS,))] * 3
                params.update(collective_id=0, has_side_effects=True)
            else:
                dkv_spec = part_spec
                dkv_shape = jax.ShapeDtypeStruct((batch,) + split, F32)
            return pl.pallas_call(
                functools.partial(attention_kernel, batch, first, last, scale=scale),
                grid=(SUBS * batch + 1 + 3 * LAG * last,),
                in_specs=in_specs,
                out_specs=[pl.BlockSpec((1, seq, wide), here), pl.BlockSpec((1, seq, wide), here), dkv_spec],
                out_shape=[jax.ShapeDtypeStruct((batch, seq, cols), BF16),
                           jax.ShapeDtypeStruct((batch, seq, cols), BF16), dkv_shape],
                scratch_shapes=scratch,
                compiler_params=pltpu.CompilerParams(**params),
                cost_estimate=pl.CostEstimate(flops=12 * tokens * cols * keys, bytes_accessed=12 * tokens * cols,
                                              transcendentals=tokens * cols // hd * keys),
                name='attend',
            )(*args)

        os, dqs, d_wos, d_wqs = [], [], [], []
        carry = None
        for n in range(CHUNKS):
            o, dq, carry = attend(n, q, d_o, carry)
            os.append(o)
            dqs.append(dq)
            d_wo = jnp.einsum('bse,bsd->ed', o, dy, preferred_element_type=F32)
            if n < CHUNKS - 1:
                d_wq = jnp.einsum('bsd,bse->de', xn, dq, preferred_element_type=F32)
                d_wo, d_wq, q, carry = lax.optimization_barrier((d_wo, d_wq, q, carry))
                d_wo, d_wq = lax.psum((d_wo, d_wq), 'sp', axis_index_groups=[[m ^ 1 for m in range(groups)]])
            else:
                d_wo, xn = lax.optimization_barrier((d_wo, xn))
                d_wo = lax.psum(d_wo, 'sp', axis_index_groups=[[m ^ 2 for m in range(groups)]])
                d_wq = jnp.einsum('bsd,bse->de', xn, dq, preferred_element_type=F32)
                dkv = carry
                rot = dkv[..., :hd].astype(BF16).astype(F32)
                rolled = jnp.concatenate([rot[..., half:], rot[..., :half]], axis=-1)
                dk_proj = (rot * cos2 - rolled * sin2).astype(BF16)
                dkv_proj = jnp.concatenate([dk_proj, dkv[..., hd:].astype(BF16)], axis=-1)
                d_wkv = jnp.einsum('bsd,bse->de', xn, dkv_proj, preferred_element_type=F32)
                d_wq, d_wkv, x_b, dy_b = lax.optimization_barrier((d_wq, d_wkv, x, dy))
                d_wq, d_wkv = lax.psum((d_wq, d_wkv), 'sp')
            d_wos.append(d_wo)
            d_wqs.append(d_wq)
        d_wo = jnp.concatenate(d_wos, axis=0)
        d_wq = jnp.concatenate(d_wqs, axis=1)

        nb2 = 2
        dx, dgain = pl.pallas_call(
            post_kernel,
            grid=(batch // nb2,),
            in_specs=[rows_spec(nb2, cols)] * CHUNKS + [
                rows_spec(nb2, 2 * hd), full(d_model, width), full(d_model, 2 * hd),
                rows_spec(nb2, d_model), rows_spec(nb2, d_model), full(1, d_model)],
            out_specs=[rows_spec(nb2, d_model), full(8, d_model)],
            out_shape=[jax.ShapeDtypeStruct((batch, seq, d_model), BF16), jax.ShapeDtypeStruct((8, d_model), F32)],
            compiler_params=pltpu.CompilerParams(vmem_limit_bytes=VMEM_LIMIT),
            cost_estimate=pl.CostEstimate(flops=2 * tokens * d_model * (width + 2 * hd),
                                          bytes_accessed=8 * tokens * d_model, transcendentals=0),
            name='norm_grad',
        )(*dqs, dkv_proj, w_q, w_kv, x_b, dy_b, gain)
        d_gain = lax.psum(jnp.sum(dgain, axis=0), 'sp')
        y = pl.pallas_call(
            out_kernel,
            grid=(batch // nb,),
            in_specs=[rows_spec(nb, cols)] * CHUNKS + [full(width, d_model), rows_spec(nb, d_model)],
            out_specs=rows_spec(nb, d_model),
            out_shape=jax.ShapeDtypeStruct((batch, seq, d_model), BF16),
            compiler_params=pltpu.CompilerParams(vmem_limit_bytes=VMEM_LIMIT),
            cost_estimate=pl.CostEstimate(flops=2 * tokens * d_model * width, bytes_accessed=6 * tokens * d_model,
                                          transcendentals=0),
            name='output',
        )(*os, w_o, x_b)
        return y, dx, d_wq, d_wkv[:, :hd], d_wkv[:, hd:], d_wo, d_gain


    return jax.shard_map(local_block, mesh=mesh, in_specs=(seq_spec, seq_spec, whole, whole, whole, whole, whole, whole), out_specs=(seq_spec, seq_spec, whole, whole, whole, whole, whole), check_vma=False)
```

```python
import functools

import jax
import jax.numpy as jnp
from jax import lax
from jax.experimental import pallas as pl
from jax.experimental.pallas import tpu as pltpu
from jax.sharding import PartitionSpec as P


ROPE_THETA = 10000.0
NORM_EPS = 1e-6
MASK_FILL = -1e30
F32 = jnp.float32
BF16 = jnp.bfloat16
MESH = pl.DeviceIdType.MESH
SUBS = (1, 3)
CHUNKS = len(SUBS)
SLOTS = 3
LAG = 3
VMEM_LIMIT = 60 * 1024 * 1024
NT = (((1,), (1,)), ((), ()))


def mm(a, b):
    return jnp.dot(a, b, preferred_element_type=F32)


def mm_nt(a, b):
    return lax.dot_general(a, b, NT, preferred_element_type=F32)


def rotate(v, cos, sin):
    return v * cos + pltpu.roll(v, v.shape[-1] // 2, 1) * sin


def norm_kernel(x_ref, gain_ref, wkv_ref, cos_ref, sin_ref, xn_ref, kv_ref):
    nb, seq, d_model = x_ref.shape
    hd = cos_ref.shape[1]
    rows = nb * seq
    x = x_ref[...].reshape(rows, d_model).astype(F32)
    inv = lax.rsqrt(jnp.mean(x * x, axis=-1, keepdims=True) + NORM_EPS)
    xn = (x * inv * (1.0 + gain_ref[...])).astype(BF16)
    xn_ref[...] = xn.reshape(nb, seq, d_model)
    cos = jnp.concatenate([cos_ref[...]] * nb, axis=0)
    sin = jnp.concatenate([sin_ref[...]] * nb, axis=0)
    kv = mm(xn, wkv_ref[...])
    kv_ref[:, :, :hd] = rotate(kv[:, :hd], cos, sin).astype(BF16).reshape(nb, seq, hd)
    kv_ref[:, :, hd:] = kv[:, hd:].astype(BF16).reshape(nb, seq, hd)


def query_kernel(xn_ref, wq_ref, cos_ref, sin_ref, q_ref, *, scale):
    nb, seq, d_model = xn_ref.shape
    hd = cos_ref.shape[1]
    xn = xn_ref[...].reshape(nb * seq, d_model)
    cos = jnp.concatenate([cos_ref[...]] * nb, axis=0)
    sin = jnp.concatenate([sin_ref[...]] * nb, axis=0)
    width = wq_ref.shape[1]
    step = 512
    for n in range(width // step):
        proj = mm(xn, wq_ref[:, n * step:(n + 1) * step])
        for h in range(step // hd):
            rot = rotate(proj[:, h * hd:(h + 1) * hd], cos, sin) * scale
            lo = n * step + h * hd
            q_ref[:, :, lo:lo + hd] = rot.astype(BF16).reshape(nb, seq, hd)


def attention_kernel(batch, subs, first, last, *refs, scale):
    refs = list(refs)
    prefix_ref, q_ref, do_ref, q_was, do_was, kv_ref, cos_ref, sin_ref = refs[:8]
    del refs[:8]
    carry_ref = None if first else refs.pop(0)
    o_ref, dq_ref, dkv_ref = refs[:3]
    s_scr, e_scr, dp_scr, k_ext, v_scr, k_t, v_t, eye_scr, top_scr, stat_scr = refs[3:13]
    if last:
        (part, recv1, sum1, recv2, sum2, recv3,
         send1, got1, send2, got2, send3, got3, free1, free2, free3) = refs[13:]
    t = pl.program_id(0)
    steps = subs * batch
    me = lax.axis_index('sp')
    core = me % 2
    x_bit = (me // 2) % 2
    y_bit = me // 4
    partner = me + 1 - 2 * core
    x_near = me + 2 - 4 * x_bit
    y_near = me + 4 - 8 * y_bit
    near_1 = x_near * (1 - core) + y_near * core
    near_2 = y_near * (1 - core) + x_near * core
    bit_1 = x_bit * (1 - core) + y_bit * core
    bit_2 = y_bit * (1 - core) + x_bit * core

    groups, _, seq, _ = kv_ref.shape
    hd = kv_ref.shape[3] // 2
    keys = groups * seq
    chunk = 256

    def copy_1(slot):
        return pltpu.make_async_remote_copy(part.at[slot, 1 - core], recv1.at[slot], send1.at[slot], got1.at[slot],
                                            device_id=(partner,), device_id_type=MESH)

    def copy_2(slot):
        return pltpu.make_async_remote_copy(sum1.at[slot, 1 - bit_1], recv2.at[slot], send2.at[slot], got2.at[slot],
                                            device_id=(near_1,), device_id_type=MESH)

    def copy_3(slot):
        return pltpu.make_async_remote_copy(sum2.at[slot, 1 - bit_2], recv3.at[slot], send3.at[slot], got3.at[slot],
                                            device_id=(near_2,), device_id_type=MESH)

    if last:
        @pl.when(t == 0)
        def _():
            barrier = pltpu.get_barrier_semaphore()
            for other in (partner, near_1, near_2):
                pl.semaphore_signal(barrier, inc=1, device_id=(other,), device_id_type=MESH)
            pl.semaphore_wait(barrier, 3)

    @pl.when(t == 0)
    def _():
        eye_scr[...] = (lax.broadcasted_iota(jnp.int32, (seq, seq), 0)
                        == lax.broadcasted_iota(jnp.int32, (seq, seq), 1)).astype(F32).astype(BF16)

    def fold(a, op):
        return op(a.reshape(chunk // 8, 8, 2 * hd), axis=0)

    def heads_of(ref, lo):
        return jnp.concatenate([ref[0, :, pl.ds(lo, hd)], ref[0, :, pl.ds(lo + hd, hd)]], axis=0)

    def masked_q(lo):
        eye = eye_scr[...]
        return jnp.concatenate([heads_of(q_ref, lo), jnp.concatenate([eye, eye], axis=0)], axis=1)

    low = functools.partial(jnp.full, (8, 2 * hd), MASK_FILL, F32)

    acc = part.at[((t + subs - 1) // subs + SLOTS - 1) % SLOTS] if last else dkv_ref.at[0]

    @pl.when((t % subs == 1 % subs) & (t <= steps))
    def _():
        acc[...] = jnp.zeros(acc.shape, F32) if first else carry_ref[0]

    @pl.when(t <= steps)
    def _():
        now, was = t % 2, (t + 1) % 2
        k_all = kv_ref[:, 0, :, :hd].reshape(keys, hd)
        v_all = kv_ref[:, 0, :, hd:].reshape(keys, hd)
        limit = jnp.maximum(prefix_ref[0, 0:1, :], me * seq + lax.broadcasted_iota(jnp.int32, (keys, seq), 1) + 1)
        k_ext[:, :hd] = k_all
        k_ext[:, hd:] = jnp.where(lax.broadcasted_iota(jnp.int32, (keys, seq), 0) < limit, 0.0, MASK_FILL).astype(BF16)
        v_scr[now] = v_all
        k_t[now] = k_all.T
        v_t[now] = v_all.T

        def score_step(i):
            buf = i
            q_ext = masked_q(i * 2 * hd)
            top = low()
            for c in range(keys // chunk):
                at = slice(c * chunk, (c + 1) * chunk)
                s = mm_nt(k_ext[at, :], q_ext)
                s_scr[buf, at, :] = s
                top = jnp.maximum(top, fold(s, jnp.max))
            top_scr[buf] = top

        def weigh_step(i, source, v_slot):
            buf = i
            do2 = heads_of(source, i * 2 * hd)
            top = jnp.max(top_scr[buf], axis=0, keepdims=True)
            total = jnp.zeros((8, 2 * hd), F32)
            cross = jnp.zeros((8, 2 * hd), F32)
            for c in range(keys // chunk):
                at = slice(c * chunk, (c + 1) * chunk)
                dp = mm_nt(v_scr[v_slot, at, :], do2).astype(BF16).astype(F32)
                e = jnp.exp(s_scr[buf, at, :] - top)
                e_scr[buf, at, :] = e
                dp_scr[buf, at, :] = dp
                total = total + fold(e, jnp.sum)
                cross = cross + fold(e * dp, jnp.sum)
            inv = 1.0 / jnp.sum(total, axis=0, keepdims=True)
            stat_scr[buf, 0:1, :] = inv
            stat_scr[buf, 1:2, :] = jnp.sum(cross, axis=0, keepdims=True) * inv

        def grad_step(i):
            buf = i
            lo = i * 2 * hd
            q2 = heads_of(q_was, lo)
            do2 = heads_of(do_was, lo)
            inv = stat_scr[buf, 0:1, :]
            delta = stat_scr[buf, 1:2, :]
            ps, dss = [], []
            for c in range(keys // chunk):
                at = slice(c * chunk, (c + 1) * chunk)
                p = e_scr[buf, at, :] * inv
                ds = (p * (dp_scr[buf, at, :] - delta)).astype(BF16)
                p = p.astype(BF16)
                ps.append(p)
                dss.append(ds)
                dk = mm(ds, q2)
                dv = mm(p, do2)
                for r in range(chunk // seq):
                    j = c * (chunk // seq) + r
                    acc[j % 2, j // 2, 0] += dk[r * seq:(r + 1) * seq, :]
                    acc[j % 2, j // 2, 1] += dv[r * seq:(r + 1) * seq, :]
            o_t = mm(v_t[was], jnp.concatenate(ps, axis=0)).astype(BF16)
            dq_t = mm(k_t[was], jnp.concatenate(dss, axis=0)).astype(BF16)
            for half in range(2):
                o_ref[0, :, pl.ds(lo + half * hd, hd)] = o_t[:, half * hd:(half + 1) * hd].T
                dq = dq_t[:, half * hd:(half + 1) * hd].T.astype(F32) * scale
                dq_ref[0, :, pl.ds(lo + half * hd, hd)] = rotate(dq, cos_ref[...], -sin_ref[...]).astype(BF16)

        score_step(0)
        weigh_step(1, do_was, was)
        grad_step(0)
        score_step(1)
        weigh_step(0, do_ref, now)
        grad_step(1)

    if not last:
        return

    def stage(number):
        ahead = t - LAG * number
        b = ahead // subs - 1
        return b, (ahead >= subs) & (ahead % subs == 0) & (b < batch)

    b4, due4 = stage(3)

    @pl.when(due4)
    def _():
        slot = b4 % SLOTS
        copy_3(slot).wait()
        done = sum2[slot, bit_2] + recv3[slot]
        dkv_ref[0, :, :hd] = done[0]
        dkv_ref[0, :, hd:] = done[1]

        @pl.when(b4 + SLOTS < batch)
        def _():
            pl.semaphore_signal(free3.at[slot], inc=1, device_id=(near_2,), device_id_type=MESH)

    b3, due3 = stage(2)

    @pl.when(due3)
    def _():
        slot = b3 % SLOTS
        copy_2(slot).wait()
        for s in range(2):
            sum2[slot, s] = sum1[slot, bit_1, s] + recv2[slot, s]

        @pl.when(b3 + SLOTS < batch)
        def _():
            pl.semaphore_signal(free2.at[slot], inc=1, device_id=(near_1,), device_id_type=MESH)

        @pl.when(b3 >= SLOTS)
        def _():
            pl.semaphore_wait(free3.at[slot], 1)

        copy_3(slot).start()

    b2, due2 = stage(1)

    @pl.when(due2)
    def _():
        slot = b2 % SLOTS
        copy_1(slot).wait()
        for f in range(2):
            for s in range(2):
                chip = f * (1 + core) + s * (2 - core)
                sum1[slot, f, s] = part[slot, core, chip] + recv1[slot, chip]

        @pl.when(b2 + SLOTS < batch)
        def _():
            pl.semaphore_signal(free1.at[slot], inc=1, device_id=(partner,), device_id_type=MESH)

        @pl.when(b2 >= SLOTS)
        def _():
            pl.semaphore_wait(free2.at[slot], 1)

        copy_2(slot).start()

    b1, due1 = stage(0)

    @pl.when(due1)
    def _():
        slot = b1 % SLOTS

        @pl.when(b1 >= SLOTS)
        def _():
            pl.semaphore_wait(free1.at[slot], 1)

        copy_1(slot).start()


def out_kernel(*refs):
    *o_refs, wo_ref, x_ref, y_ref = refs
    nb, seq, d_model = x_ref.shape
    rows = nb * seq
    o = jnp.concatenate([r[...].reshape(rows, r.shape[2]) for r in o_refs], axis=1)
    step = 512
    for n in range(d_model // step):
        at = slice(n * step, (n + 1) * step)
        x = x_ref[:, :, at].reshape(rows, step).astype(F32)
        y_ref[:, :, at] = (x + mm(o, wo_ref[:, at])).astype(BF16).reshape(nb, seq, step)


def post_kernel(*refs):
    *dq_refs, dkv_ref, wq_ref, wkv_ref, x_ref, dy_ref, gain_ref, dx_ref, dgain_ref = refs
    nb, seq, d_model = x_ref.shape
    rows = nb * seq
    dq = jnp.concatenate([r[...].reshape(rows, r.shape[2]) for r in dq_refs], axis=1)
    acc = mm_nt(dq, wq_ref[...])
    acc = acc + mm_nt(dkv_ref[...].reshape(rows, dkv_ref.shape[2]), wkv_ref[...])
    g = acc.astype(BF16).astype(F32)
    x = x_ref[...].reshape(rows, d_model).astype(F32)
    inv = lax.rsqrt(jnp.mean(x * x, axis=-1, keepdims=True) + NORM_EPS)
    xr = x * inv
    part = jnp.sum((g * xr).reshape(rows // 8, 8, d_model), axis=0)
    u = g * (1.0 + gain_ref[...])
    mean = jnp.mean(u * xr, axis=-1, keepdims=True)
    dy = dy_ref[...].reshape(rows, d_model).astype(F32)
    dx_ref[...] = (dy + inv * (u - xr * mean)).astype(BF16).reshape(nb, seq, d_model)

    @pl.when(pl.program_id(0) == 0)
    def _():
        dgain_ref[...] = jnp.zeros_like(dgain_ref)

    dgain_ref[...] += part


def solution(mesh):
    groups = mesh.shape['sp']
    seq_spec = P(None, 'sp', None)
    whole = P()

    def local_block(x, dy, prefix_len, w_norm, w_q, w_k, w_v, w_o):
        batch, seq, d_model = x.shape
        hd = w_k.shape[1]
        width = w_q.shape[1]
        keys = seq * groups
        tokens = batch * seq
        scale = hd ** -0.5
        me = lax.axis_index('sp')
        half = hd // 2
        freq = ROPE_THETA ** (-2.0 * jnp.arange(half, dtype=F32) / hd)
        angles = (me * seq + jnp.arange(seq)).astype(F32)[:, None] * freq[None, :]
        cos, sin = jnp.cos(angles), jnp.sin(angles)
        cos2 = jnp.concatenate([cos, cos], axis=1)
        sin2 = jnp.concatenate([-sin, sin], axis=1)
        gain = w_norm.astype(F32).reshape(1, d_model)
        w_kv = jnp.concatenate([w_k, w_v], axis=1)

        nb = 4

        def rows_spec(n, w):
            return pl.BlockSpec((n, seq, w), lambda i: (i, 0, 0))

        def full(*shape):
            return pl.BlockSpec(shape, lambda i: (0,) * len(shape))

        xn, kv = pl.pallas_call(
            norm_kernel,
            grid=(batch // nb,),
            in_specs=[rows_spec(nb, d_model), full(1, d_model), full(d_model, 2 * hd), full(seq, hd), full(seq, hd)],
            out_specs=[rows_spec(nb, d_model), rows_spec(nb, 2 * hd)],
            out_shape=[jax.ShapeDtypeStruct((batch, seq, d_model), BF16),
                       jax.ShapeDtypeStruct((batch, seq, 2 * hd), BF16)],
            compiler_params=pltpu.CompilerParams(vmem_limit_bytes=VMEM_LIMIT),
            cost_estimate=pl.CostEstimate(flops=4 * tokens * d_model * hd, bytes_accessed=4 * tokens * d_model,
                                          transcendentals=0),
            name='norm',
        )(x, gain, w_kv, cos2, sin2)
        kv_all = lax.all_gather(kv, 'sp', axis=0, tiled=False)
        q = pl.pallas_call(
            functools.partial(query_kernel, scale=scale),
            grid=(batch // nb,),
            in_specs=[rows_spec(nb, d_model), full(d_model, width), full(seq, hd), full(seq, hd)],
            out_specs=rows_spec(nb, width),
            out_shape=jax.ShapeDtypeStruct((batch, seq, width), BF16),
            compiler_params=pltpu.CompilerParams(vmem_limit_bytes=VMEM_LIMIT),
            cost_estimate=pl.CostEstimate(flops=2 * tokens * d_model * width, bytes_accessed=4 * tokens * d_model,
                                          transcendentals=0),
            name='query',
        )(xn, w_q, cos2, sin2)
        d_o = jnp.einsum('bsd,ed->bse', dy, w_o, preferred_element_type=F32).astype(BF16)

        f32_tile = (seq, hd)
        prefix = jnp.broadcast_to(prefix_len[:, None, None], (batch, 8, hd))
        wide = width // sum(SUBS)
        split = (2, groups // 2, 2) + f32_tile

        def attend(n, q, d_o, carry):
            first, last = n == 0, n == CHUNKS - 1
            subs, skip = SUBS[n], sum(SUBS[:n])
            cols = subs * wide
            top = subs * batch - 1
            now = lambda i: jnp.minimum(i, top)
            before = lambda i: jnp.clip(i - 1, 0, top)
            here = lambda i: (before(i) // subs, 0, before(i) % subs)
            part_spec = pl.BlockSpec((1,) + split, lambda i: (before(i) // subs, 0, 0, 0, 0, 0))
            at_now = pl.BlockSpec((1, seq, wide), lambda i: (now(i) // subs, 0, skip + now(i) % subs))
            at_before = pl.BlockSpec((1, seq, wide), lambda i: (before(i) // subs, 0, skip + before(i) % subs))
            in_specs = [pl.BlockSpec((1, 8, hd), lambda i: (now(i) // subs, 0, 0)),
                        at_now, at_now, at_before, at_before,
                        pl.BlockSpec((groups, 1, seq, 2 * hd), lambda i: (0, now(i) // subs, 0, 0)),
                        full(seq, hd), full(seq, hd)]
            args = [prefix, q, d_o, q, d_o, kv_all, cos2, sin2]
            if not first:
                in_specs.append(part_spec)
                args.append(carry)
            scratch = [
                pltpu.VMEM((2, keys, 2 * hd), F32), pltpu.VMEM((2, keys, 2 * hd), F32), pltpu.VMEM((2, keys, 2 * hd), F32),
                pltpu.VMEM((keys, 2 * hd), BF16), pltpu.VMEM((2, keys, hd), BF16),
                pltpu.VMEM((2, hd, keys), BF16), pltpu.VMEM((2, hd, keys), BF16),
                pltpu.VMEM((seq, seq), BF16), pltpu.VMEM((2, 8, 2 * hd), F32), pltpu.VMEM((2, 8, 2 * hd), F32)]
            params = dict(vmem_limit_bytes=VMEM_LIMIT)
            if last:
                dkv_spec = pl.BlockSpec((1, seq, 2 * hd), lambda i: (jnp.maximum(i - subs - 3 * LAG, 0) // subs, 0, 0))
                dkv_shape = jax.ShapeDtypeStruct((batch, seq, 2 * hd), F32)
                scratch += [pltpu.VMEM((SLOTS,) + shape + f32_tile, F32) for shape in
                            ((2, groups // 2, 2), (4, 2), (2, 2, 2), (2, 2), (2, 2), (2,))]
                scratch += [pltpu.SemaphoreType.DMA((SLOTS,))] * 6 + [pltpu.SemaphoreType.REGULAR((SLOTS,))] * 3
                params.update(collective_id=0, has_side_effects=True)
            else:
                dkv_spec = part_spec
                dkv_shape = jax.ShapeDtypeStruct((batch,) + split, F32)
            return pl.pallas_call(
                functools.partial(attention_kernel, batch, subs, first, last, scale=scale),
                grid=(subs * batch + 1 + 3 * LAG * last,),
                in_specs=in_specs,
                out_specs=[pl.BlockSpec((1, seq, wide), here), pl.BlockSpec((1, seq, wide), here), dkv_spec],
                out_shape=[jax.ShapeDtypeStruct((batch, seq, cols), BF16),
                           jax.ShapeDtypeStruct((batch, seq, cols), BF16), dkv_shape],
                scratch_shapes=scratch,
                compiler_params=pltpu.CompilerParams(**params),
                cost_estimate=pl.CostEstimate(flops=12 * tokens * cols * keys, bytes_accessed=12 * tokens * cols,
                                              transcendentals=tokens * cols // hd * keys),
                name='attend',
            )(*args)

        os, dqs, d_wos, d_wqs = [], [], [], []
        carry = None
        for n in range(CHUNKS):
            o, dq, carry = attend(n, q, d_o, carry)
            os.append(o)
            dqs.append(dq)
            d_wo = jnp.einsum('bse,bsd->ed', o, dy, preferred_element_type=F32)
            if n < CHUNKS - 1:
                d_wq = jnp.einsum('bsd,bse->de', xn, dq, preferred_element_type=F32)
                d_wo, d_wq, q, carry = lax.optimization_barrier((d_wo, d_wq, q, carry))
                d_wo, d_wq = lax.psum((d_wo, d_wq), 'sp', axis_index_groups=[[m ^ 1 for m in range(groups)]])
            else:
                d_wo, xn = lax.optimization_barrier((d_wo, xn))
                d_wo = lax.psum(d_wo, 'sp', axis_index_groups=[[m ^ 2 for m in range(groups)]])
                d_wq = jnp.einsum('bsd,bse->de', xn, dq, preferred_element_type=F32)
                dkv = carry
                rot = dkv[..., :hd].astype(BF16).astype(F32)
                rolled = jnp.concatenate([rot[..., half:], rot[..., :half]], axis=-1)
                dk_proj = (rot * cos2 - rolled * sin2).astype(BF16)
                dkv_proj = jnp.concatenate([dk_proj, dkv[..., hd:].astype(BF16)], axis=-1)
                d_wkv = jnp.einsum('bsd,bse->de', xn, dkv_proj, preferred_element_type=F32)
                d_wq, d_wkv, x_b, dy_b = lax.optimization_barrier((d_wq, d_wkv, x, dy))
                d_wq, d_wkv = lax.psum((d_wq, d_wkv), 'sp')
            d_wos.append(d_wo)
            d_wqs.append(d_wq)
        d_wo = jnp.concatenate(d_wos, axis=0)
        d_wq = jnp.concatenate(d_wqs, axis=1)

        nb2 = 2
        dx, dgain = pl.pallas_call(
            post_kernel,
            grid=(batch // nb2,),
            in_specs=[rows_spec(nb2, c * wide) for c in SUBS] + [
                rows_spec(nb2, 2 * hd), full(d_model, width), full(d_model, 2 * hd),
                rows_spec(nb2, d_model), rows_spec(nb2, d_model), full(1, d_model)],
            out_specs=[rows_spec(nb2, d_model), full(8, d_model)],
            out_shape=[jax.ShapeDtypeStruct((batch, seq, d_model), BF16), jax.ShapeDtypeStruct((8, d_model), F32)],
            compiler_params=pltpu.CompilerParams(vmem_limit_bytes=VMEM_LIMIT),
            cost_estimate=pl.CostEstimate(flops=2 * tokens * d_model * (width + 2 * hd),
                                          bytes_accessed=8 * tokens * d_model, transcendentals=0),
            name='norm_grad',
        )(*dqs, dkv_proj, w_q, w_kv, x_b, dy_b, gain)
        d_gain = lax.psum(jnp.sum(dgain, axis=0), 'sp')
        y = pl.pallas_call(
            out_kernel,
            grid=(batch // nb,),
            in_specs=[rows_spec(nb, c * wide) for c in SUBS] + [full(width, d_model), rows_spec(nb, d_model)],
            out_specs=rows_spec(nb, d_model),
            out_shape=jax.ShapeDtypeStruct((batch, seq, d_model), BF16),
            compiler_params=pltpu.CompilerParams(vmem_limit_bytes=VMEM_LIMIT),
            cost_estimate=pl.CostEstimate(flops=2 * tokens * d_model * width, bytes_accessed=6 * tokens * d_model,
                                          transcendentals=0),
            name='output',
        )(*os, w_o, x_b)
        return y, dx, d_wq, d_wkv[:, :hd], d_wkv[:, hd:], d_wo, d_gain


    return jax.shard_map(local_block, mesh=mesh, in_specs=(seq_spec, seq_spec, whole, whole, whole, whole, whole, whole), out_specs=(seq_spec, seq_spec, whole, whole, whole, whole, whole), check_vma=False)
```
